32 devices in a mesh: chain: 4 (over x, core), blk: 8 (over z, y).
Axes of the slice: x: 2, y: 2, z: 4, core: 2. Of those that a mesh axis runs over, the one named last changes fastest.
Arguments:
- schur: bfloat16 [8192, 2048], P(('chain', 'blk')), as said below
- coupling: bfloat16 [8192, 2048], P(('chain', 'blk')), may hold values from -0.0625 to 0.0625
- next_diag: float32 [8192, 2048], P(('chain', 'blk')), as said below
Outputs:
- factor: float32 [8192, 2048], P(('chain', 'blk'))
- next_schur: float32 [8192, 2048], P(('chain', 'blk'))
The draws below stay inside these ranges and needn't reach their ends.
Inputs may be any that keep to these rules, and one draw needn't show every extreme that they name: `schur`: every slab's block is symmetric positive definite. `next_diag`: every slab's block is symmetric positive definite.
All inputs are finite; a program needn't handle non-finite values.
Results may differ from the reference program's by a relative error of at most 0.0034.
Values may be sent and summed in bfloat16 or wider, within the bound.
A program may use at most 128 MiB of HBM per device.

```python
import jax
import jax.numpy as jnp
from jax import lax

NB = 2048
SLABS = 4


def spd_slabs(key, floor_value):
    noise_key, shift_key = jax.random.split(key)
    raw = jax.random.normal(noise_key, (SLABS, NB, NB), jnp.float32)
    floor_part = floor_value * (1.0 + 0.5 * jax.random.uniform(shift_key, (SLABS, NB), jnp.float32))
    gram = jnp.einsum('sij,skj->sik', raw, raw, precision=lax.Precision.HIGHEST) / jnp.float32(NB)
    matrix = gram + floor_part[:, :, None] * jnp.eye(NB, dtype=jnp.float32)[None, :, :]
    return matrix.reshape(SLABS * NB, NB)


def draw_schur(key, part):
    return spd_slabs(jax.random.fold_in(key, 11), 0.02).astype(jnp.bfloat16)


def draw_next_diag(key, part):
    return spd_slabs(jax.random.fold_in(key, 23), 2.0)


def steps_of(own_key, shape, pieces, least, largest):
    level, own = 1.0, jax.random.fold_in(own_key, 6)
    for axis_at, parts in pieces:
        steps = jnp.exp(jax.random.uniform(jax.random.fold_in(own, axis_at), (parts,), jnp.float32, least / len(pieces), largest / len(pieces)))
        level = level * jnp.repeat(steps, shape[axis_at] // parts).reshape([-1 if axis == axis_at else 1 for axis in range(len(shape))])
    return level


def normal_values(key, dims, spread, most, shards=(), held_as=jnp.bfloat16):
    gain = steps_of(key, dims, shards, -0.22, 0.18) if shards else 1.0
    values = jax.random.normal(key, dims, jnp.float32) * spread * gain
    return jnp.minimum(jnp.maximum(values, -most), most).astype(held_as)


def setup_inputs(seed: int = 0) -> dict:
    keys = jax.random.split(jax.random.key(seed), 4)
    return {
        "schur": draw_schur(jax.random.fold_in(keys[3], 71), 0),
        "coupling": normal_values(keys[1], (SLABS * NB, NB), (4 * NB) ** -0.5, 0.0625, ((0, 32),)),
        "next_diag": draw_next_diag(jax.random.fold_in(keys[3], 71), 0),
    }


def factor_slab(blocks_pair):
    diag_block, couple_block = blocks_pair
    lower = jnp.linalg.cholesky(diag_block.astype(jnp.float32))
    solved = lax.linalg.triangular_solve(lower, couple_block.astype(jnp.float32).T, left_side=True, lower=True).astype(jnp.bfloat16)
    update = jnp.dot(solved.T.astype(jnp.float32), solved.astype(jnp.float32), preferred_element_type=jnp.float32)
    return (lower, update)

def reference(schur, coupling, next_diag):
    blocks = schur.reshape(SLABS, NB, NB)
    couple = coupling.reshape(SLABS, NB, NB)
    factors, updates = lax.map(factor_slab, (blocks, couple))
    shifted = jnp.concatenate([jnp.zeros((1, NB, NB), jnp.float32), updates[:-1]], axis=0)
    fresh = next_diag.reshape(SLABS, NB, NB) - shifted
    return (factors.reshape(SLABS * NB, NB), fresh.reshape(SLABS * NB, NB))
```

```python
import functools
import jax
import jax.numpy as jnp
from jax import lax
from jax.experimental import pallas as pl
from jax.experimental.pallas import tpu as pltpu

B = 128
BF = jnp.bfloat16
F32 = jnp.float32


def split(x):
    hi = x.astype(BF)
    return hi, (x - hi.astype(F32)).astype(BF)


def dot_t(a, b):
    return lax.dot_general(a, b, (((1,), (1,)), ((), ())), preferred_element_type=F32)


def eliminate(block):
    size = block.shape[0]
    count = size // 8
    sub = lax.broadcasted_iota(jnp.int32, (8, size), 0)
    lane = lax.broadcasted_iota(jnp.int32, (8, size), 1)
    rows = [block[8 * t : 8 * t + 8, :] for t in range(count)]
    inv = [jnp.where(lane == sub + 8 * t, 1.0, 0.0).astype(F32) for t in range(count)]
    for k in range(size):
        s, r = divmod(k, 8)
        row_a = jnp.broadcast_to(rows[s][r : r + 1, :], (8, size))
        row_n = jnp.broadcast_to(inv[s][r : r + 1, :], (8, size))
        pivot = jnp.broadcast_to(row_a[:, k : k + 1], (8, size))
        scale = lax.rsqrt(pivot)
        u_a = row_a * scale
        u_n = row_n * scale
        w_a = u_a * scale
        w_n = u_n * scale
        for t in range(s, count):
            c = jnp.broadcast_to(rows[t][:, k : k + 1], (8, size))
            if t == s:
                keep = sub > r
                c = jnp.where(keep, c, 0.0)
                here = sub == r
                rows[t] = jnp.where(here, u_a, rows[t] - c * w_a)
                inv[t] = jnp.where(here, u_n, inv[t] - c * w_n)
            else:
                rows[t] = rows[t] - c * w_a
                inv[t] = inv[t] - c * w_n
    return jnp.concatenate(rows, 0), jnp.concatenate(inv, 0)


def factor_kernel(total, s_ref, c_ref, f_ref, y_ref, work, left, right):
    extra = c_ref.shape[0]
    panels = total // B
    T = 256
    me = lax.axis_index("blk")

    def load(i, _):
        at = pl.multiple_of(i * T, T)
        work[pl.ds(at, T), :] = s_ref[pl.ds(at, T), :].astype(F32)
        return 0

    lax.fori_loop(0, total // T, load, 0)
    work[pl.ds(total, extra), :] = c_ref[...].astype(F32)
    f_ref[...] = jnp.zeros_like(f_ref)
    tri = lax.broadcasted_iota(jnp.int32, (B, B), 0) >= lax.broadcasted_iota(jnp.int32, (B, B), 1)

    def panel(p, _):
        at = pl.multiple_of(p * B, B)
        col = pl.ds(at, B)
        upper, inv = eliminate(work[col, col])
        ih, il = split(inv)
        first = p * B // T
        inv3 = jnp.concatenate([ih, il, ih], 1)

        def solve(i, _):
            rr = pl.ds(pl.multiple_of(i * T, T), T)
            bh, bl = split(work[rr, col])
            x = dot_t(jnp.concatenate([bh, bh, bl], 1), inv3)
            work[rr, col] = x
            xh, xl = split(x)
            left[rr, :] = jnp.concatenate([xh, xh, xl], 1)
            right[rr, :] = jnp.concatenate([xh, xl, xh], 1)
            return 0

        lax.fori_loop(first, (total + extra) // T, solve, 0)
        work[col, col] = jnp.where(tri, upper.T, 0.0)

        def update_col(j, _):
            cc = pl.ds(pl.multiple_of(j * T, T), T)
            b = right[cc, :]

            def update(i, _):
                rr = pl.ds(pl.multiple_of(i * T, T), T)
                work[rr, cc] = work[rr, cc] - dot_t(left[rr, :], b)
                return 0

            lax.fori_loop(j, (total + extra) // T, update, 0)
            return 0

        if True:
            @pl.when(p % 2 == 0)
            def _():
                half = pl.ds(pl.multiple_of(at + B, B), B)
                b = right[half, :]

                def update(i, _):
                    rr = pl.ds(pl.multiple_of(i * T, T), T)
                    work[rr, half] = work[rr, half] - dot_t(left[rr, :], b)
                    return 0

                lax.fori_loop(first, (total + extra) // T, update, 0)

        lax.fori_loop(first + 1, total // T, update_col, 0)
        return 0

    lax.fori_loop(0, panels, panel, 0)
    f_ref[...] = work[pl.ds(pl.multiple_of(me * extra, extra), extra), :]
    for q in range(total // B):
        @pl.when(q * B >= (me + 1) * extra)
        def _():
            f_ref[:, q * B : (q + 1) * B] = jnp.zeros((extra, B), F32)
        if True:
            rowi = me * extra + lax.broadcasted_iota(jnp.int32, (extra, B), 0)
            coli = q * B + lax.broadcasted_iota(jnp.int32, (extra, B), 1)
            f_ref[:, q * B : (q + 1) * B] = jnp.where(rowi >= coli, f_ref[:, q * B : (q + 1) * B], 0.0)
    y_ref[...] = work[pl.ds(total, extra), :].astype(BF)


def factor_call(s, c):
    total, extra = s.shape[1], c.shape[0]
    return pl.pallas_call(
        functools.partial(factor_kernel, total),
        out_shape=(jax.ShapeDtypeStruct((extra, total), F32), jax.ShapeDtypeStruct((extra, total), BF)),
        in_specs=[pl.BlockSpec(memory_space=pltpu.VMEM)] * 2,
        out_specs=(pl.BlockSpec(memory_space=pltpu.VMEM), pl.BlockSpec(memory_space=pltpu.VMEM)),
        scratch_shapes=[
            pltpu.VMEM((total + extra, total), F32),
            pltpu.VMEM((total + extra, 3 * B), BF),
            pltpu.VMEM((total + extra, 3 * B), BF),
        ],
        compiler_params=pltpu.CompilerParams(vmem_limit_bytes=60 * 1024 * 1024),
        name="factor_slab",
    )(s, c)
from jax.sharding import PartitionSpec as P


def passed_along(value, axis, steps):
    count = lax.axis_size(axis)
    initial, last = (max(0, -steps), min(count, count - steps))
    return lax.ppermute(value, axis, [(source, source + steps) for source in range(initial, last)])


def local(schur, coupling, next_diag):
    whole = lax.all_gather(schur, "blk", axis=0, tiled=True)
    my_rows, solved = factor_call(whole, coupling)
    arrived = passed_along(solved, "chain", 1)
    every = lax.all_gather(arrived, "blk", axis=0, tiled=True)
    return (my_rows, next_diag - dot_t(arrived, every))


def solution(mesh):
    placed = (P(("chain", "blk"), None),) * 3
    return jax.shard_map(
        local, mesh=mesh, in_specs=placed, out_specs=(P(("chain", "blk"), None),) * 2, check_vma=False
    )
```

```python
import functools
import jax
import jax.numpy as jnp
from jax import lax
from jax.experimental import pallas as pl
from jax.experimental.pallas import tpu as pltpu
from jax.sharding import PartitionSpec as P

B = 128
BF = jnp.bfloat16
F32 = jnp.float32


def split(x):
    hi = x.astype(BF)
    return hi, (x - hi.astype(F32)).astype(BF)


def dot_t(a, b):
    return lax.dot_general(a, b, (((1,), (1,)), ((), ())), preferred_element_type=F32)


def eliminate(block):
    size = block.shape[0]
    count = size // 8
    sub = lax.broadcasted_iota(jnp.int32, (8, size), 0)
    lane = lax.broadcasted_iota(jnp.int32, (8, size), 1)
    rows = [block[8 * t : 8 * t + 8, :] for t in range(count)]
    inv = [jnp.where(lane == sub + 8 * t, 1.0, 0.0).astype(F32) for t in range(count)]
    group = 4

    def lane_of(x, k):
        return jnp.broadcast_to(x[:, k : k + 1], (8, size))

    def row_of(x, r):
        return jnp.broadcast_to(x[r : r + 1, :], (8, size))

    for k in range(0, size, group):
        s, r = divmod(k, 8)
        span = range(group)
        u = [row_of(rows[s], r + i) for i in span]
        n = [row_of(inv[s], r + i) for i in span]
        pivot = [[lane_of(u[i], k + j) if j >= i else None for j in span] for i in span]
        scale = [None] * group
        for i in span:
            scale[i] = lax.rsqrt(pivot[i][i])
            u[i] = u[i] * scale[i]
            n[i] = n[i] * scale[i]
            for j in range(i + 1, group):
                pivot[i][j] = pivot[i][j] * scale[i]
            for j in range(i + 1, group):
                u[j] = u[j] - pivot[i][j] * u[i]
                n[j] = n[j] - pivot[i][j] * n[i]
                for m in range(j, group):
                    pivot[j][m] = pivot[j][m] - pivot[i][j] * pivot[i][m]
        for t in range(s, count):
            if t == s and r + group == 8:
                new_a, new_n = rows[t], inv[t]
            else:
                c = [lane_of(rows[t], k + i) for i in span]
                new_a, new_n = rows[t], inv[t]
                for i in span:
                    x = c[i] * scale[i]
                    for j in range(i + 1, group):
                        c[j] = c[j] - x * pivot[i][j]
                    if t == s:
                        x = jnp.where(sub >= r + group, x, 0.0)
                    new_a = new_a - x * u[i]
                    new_n = new_n - x * n[i]
            if t == s:
                for i in span:
                    new_a = jnp.where(sub == r + i, u[i], new_a)
                    new_n = jnp.where(sub == r + i, n[i], new_n)
            rows[t], inv[t] = new_a, new_n
    return jnp.concatenate(rows, 0), jnp.concatenate(inv, 0)


def chunk_kernel(total, start, s_ref, c_ref, *refs):
    priors = refs[:-6]
    x_ref, f_ref, y_ref, work, left, right = refs[-6:]
    extra, width = c_ref.shape
    T = 2 * B
    me = lax.axis_index("blk")
    tail = pl.ds(total, extra)
    own = pl.ds(start, width)

    def tile(i):
        return pl.ds(pl.multiple_of(i * T, T), T)

    def over_rows(first, visit):
        def step(i, _):
            visit(tile(i))
            return 0

        lax.fori_loop(first, total // T, step, 0)
        visit(tail)

    def bring(rr, value):
        for prior in priors:
            hi, lo = prior[rr, :width], prior[rr, width:]
            own_hi, own_lo = prior[own, :width], prior[own, width:]
            value = value - (dot_t(hi, own_hi) + (dot_t(hi, own_lo) + dot_t(lo, own_hi)))
        work[rr, :] = value

    def load(i, _):
        bring(tile(i), s_ref[tile(i), :].astype(F32))
        return 0

    lax.fori_loop(start // T, total // T, load, 0)
    bring(tail, c_ref[...].astype(F32))
    tri = lax.broadcasted_iota(jnp.int32, (B, B), 0) >= lax.broadcasted_iota(jnp.int32, (B, B), 1)

    def panel(p, _):
        at = pl.multiple_of(p * B, B)
        here = pl.ds(pl.multiple_of(start + at, B), B)
        col = pl.ds(at, B)
        low_col = pl.ds(pl.multiple_of(width + at, B), B)
        slot = pl.ds(pl.multiple_of((p % 2) * 3 * B, 3 * B), 3 * B)
        upper, inv = eliminate(work[here, col])
        ih, il = split(inv)
        inv3 = jnp.concatenate([ih, il, ih], 1)
        first = start // T + p // 2

        def solve(rr):
            bh, bl = split(work[rr, col])
            x = dot_t(jnp.concatenate([bh, bh, bl], 1), inv3)
            work[rr, col] = x
            xh, xl = split(x)
            left[rr, slot] = jnp.concatenate([xh, xh, xl], 1)
            right[rr, slot] = jnp.concatenate([xh, xl, xh], 1)
            x_ref[rr, col] = xh
            x_ref[rr, low_col] = xl

        over_rows(first, solve)
        work[here, col] = jnp.where(tri, upper.T, 0.0)

        @pl.when(p % 2 == 0)
        def _():
            half = pl.ds(pl.multiple_of(at + B, B), B)
            b = right[pl.ds(pl.multiple_of(start + at + B, B), B), : 3 * B]

            def update(rr):
                work[rr, half] = work[rr, half] - dot_t(left[rr, : 3 * B], b)

            over_rows(first, update)

        @pl.when(p % 2 == 1)
        def _():
            def update_col(j, _):
                b = right[pl.ds(pl.multiple_of(start + j * T, T), T), :]

                def update(rr):
                    work[rr, tile(j)] = work[rr, tile(j)] - dot_t(left[rr, :], b)

                over_rows(start // T + j, update)
                return 0

            lax.fori_loop(p // 2 + 1, width // T, update_col, 0)

        return 0

    lax.fori_loop(0, width // B, panel, 0)
    row = me * extra + lax.broadcasted_iota(jnp.int32, (extra, width), 0)
    column = start + lax.broadcasted_iota(jnp.int32, (extra, width), 1)
    mine = work[pl.ds(pl.multiple_of(me * extra, extra), extra), :]
    f_ref[...] = jnp.where(row >= column, mine, 0.0)
    y_ref[...] = work[tail, :].astype(BF)


def chunk_call(start, s, c, priors):
    total, (extra, width) = s.shape[0], c.shape
    every = total + extra
    live = every - start
    vmem = pl.BlockSpec(memory_space=pltpu.VMEM)
    return pl.pallas_call(
        functools.partial(chunk_kernel, total, start),
        out_shape=(
            jax.ShapeDtypeStruct((every, 2 * width), BF),
            jax.ShapeDtypeStruct((extra, width), F32),
            jax.ShapeDtypeStruct((extra, width), BF),
        ),
        in_specs=[vmem] * (2 + len(priors)),
        out_specs=(vmem, vmem, vmem),
        scratch_shapes=[
            pltpu.VMEM((every, width), F32),
            pltpu.VMEM((every, 6 * B), BF),
            pltpu.VMEM((every, 6 * B), BF),
        ],
        compiler_params=pltpu.CompilerParams(vmem_limit_bytes=56 * 1024 * 1024),
        cost_estimate=pl.CostEstimate(flops=COST, bytes_accessed=8 * live * width, transcendentals=0),
        name="factor_chunk",
    )(s, c, *priors)


COST = 50000000000


def passed_along(value, axis, steps):
    count = lax.axis_size(axis)
    initial, last = (max(0, -steps), min(count, count - steps))
    return lax.ppermute(value, axis, [(source, source + steps) for source in range(initial, last)])


def local(schur, coupling, next_diag):
    total = schur.shape[1]
    width = max(total // 4, 2 * B)
    starts = range(0, total, width)
    early = lax.all_gather(schur[:, :width], "blk", axis=0, tiled=True)
    late = lax.all_gather(schur[:, width:], "blk", axis=0, tiled=True)
    wholes = [early] + [late[:, at - width : at] for at in starts[1:]]
    priors, factors = [], []
    fresh, waiting = next_diag, None
    for at, whole in zip(starts, wholes):
        held, rows, solved = chunk_call(at, whole, coupling[:, at : at + width], priors)
        priors.append(held)
        factors.append(rows)
        arrived = passed_along(solved, "chain", 1)
        priors, arrived = lax.optimization_barrier((priors, arrived))
        if waiting is not None:
            fresh = fresh - dot_t(*waiting)
            priors, fresh = lax.optimization_barrier((priors, fresh))
        waiting = (arrived, lax.all_gather(arrived, "blk", axis=0, tiled=True))
    fresh = fresh - dot_t(*waiting)
    return (jnp.concatenate(factors, axis=1), fresh)


def solution(mesh):
    placed = (P(("chain", "blk"), None),) * 3
    return jax.shard_map(
        local, mesh=mesh, in_specs=placed, out_specs=(P(("chain", "blk"), None),) * 2, check_vma=False
    )
```
